32 devices in a mesh: group: 2 (over x), tensoror: 4 (over z), seq: 4 (over y, core).
Axes of the slice: x: 2, y: 2, z: 4, core: 2. Of those that a mesh axis runs over, the one named last changes fastest.
Arguments:
- visual_hidden: bfloat16 [16, 512, 5120], P('group', 'seq', 'tensoror'), may hold values from -6 to 6
- projector_weight: bfloat16 [5120, 5120], P('tensoror'), may hold values from -0.078125 to 0.078125
- text_embeddings: bfloat16 [16, 2048, 5120], P(('group', 'tensoror'), 'seq'), may hold values from -6 to 6
- tile_counts: int32 [16], replicated, may hold values from 1 to 2, 24 in all
- image_start: int32 [16], replicated, may hold values from 0 to 1536
- norm_gain: float32 [5120], replicated, may hold values from 0.5 to 1.5
- query_weight: bfloat16 [5120, 2560], P('tensoror'), may hold values from -3 to 3
- keyvalue_weight: bfloat16 [5120, 1024], P('tensoror'), may hold values from -0.08385255 to 0.08385255
Outputs:
- context: bfloat16 [16, 2048, 2560], P(('group', 'tensoror'), 'seq')
The draws below stay inside these ranges and needn't reach their ends.
Inputs may be any that keep to these rules, and one draw needn't show every extreme that they name: `tile_counts`: the counts of all sequences sum to 24.
All inputs are finite; a program needn't handle non-finite values.
Results may differ from the reference program's by a relative error of at most 0.0061.
Values may be sent and summed in bfloat16 or wider, within the bound.
No kernel may reach another device: no remote copies, remote signals or barrier semaphores. Data moves between devices by JAX's collectives and lax.ppermute only.
A program may use at most 192 MiB of HBM per device.

```python
import math
import jax
import jax.numpy as jnp
import numpy as np
from jax import lax

MODEL_WIDTH = 5120
QUERY_HEADS = 20
KEY_VALUE_HEADS = 4
HEAD_SIZE = 128
SEQUENCE_LENGTH = 2048
TILE = 256
MAXT = 2
SEQUENCE_COUNT = 16
MAXV = 512
TILES = 24


def weight_draws(key):
    bound = 6.0 / math.sqrt(MODEL_WIDTH)
    starting_query = jax.random.normal(jax.random.fold_in(key, 101), (MODEL_WIDTH, QUERY_HEADS * HEAD_SIZE), jnp.float32) / math.sqrt(MODEL_WIDTH)
    starting_pair = jax.random.normal(jax.random.fold_in(key, 202), (MODEL_WIDTH, 2 * KEY_VALUE_HEADS * HEAD_SIZE), jnp.float32) / math.sqrt(MODEL_WIDTH)
    return (jnp.clip(starting_query, -bound, bound), jnp.clip(starting_pair, -bound, bound))


def draw_query_weight(key, part):
    starting_query, starting_pair = weight_draws(key)
    return starting_query.astype(jnp.bfloat16)


def draw_keyvalue_weight(key, part):
    starting_query, starting_pair = weight_draws(key)
    return starting_pair.astype(jnp.bfloat16)


def place_ends(array, key, smallest, top_value):
    longest = array.shape.index(max(array.shape))
    spots = []
    for shift in (0, 1):
        where = [jax.random.randint(jax.random.fold_in(key, axis), (), 0, length) for axis, length in enumerate(array.shape)]
        where[longest] = (where[longest] + shift) % array.shape[longest]
        spots.append(tuple(where))
    return array.at[spots[0]].set(smallest).at[spots[1]].set(top_value)


def steps_of(key, extent, shards, smallest, largest):
    factor_of = 1.0
    for axis_at, shards_of in shards:
        heights = jax.random.uniform(jax.random.fold_in(jax.random.fold_in(key, 6), axis_at), (shards_of,), jnp.float32, smallest / len(shards), largest / len(shards))
        factor_of = factor_of * jnp.repeat(jnp.exp(heights), extent[axis_at] // shards_of).reshape((-1,) + (1,) * (len(extent) - 1 - axis_at))
    return factor_of


def length_profile(number_of, total, limit, slope):
    loads = [(1 << 20) // math.isqrt(grade ** slope) + 1 for grade in range(2, number_of + 1)]
    surplus, holding = total - limit - (number_of - 1), [1] * (number_of - 1)
    while surplus > 0:
        free = [i for i in range(number_of - 1) if holding[i] < limit]
        pool, remaining = sum([loads[i] for i in free]), surplus
        for i in free:
            addition = min(limit - holding[i], max(1, remaining * loads[i] // pool), surplus)
            holding[i] = holding[i] + addition
            surplus = surplus - addition
    return np.array([limit] + holding)


def uneven(key, amount, total, limit, skew):
    if amount == 2:
        one = jax.random.randint(key, (), max(1, total - limit), min(limit, total - 1) + 1)
        return jnp.stack([one, total - one])
    sizes = jnp.asarray(length_profile(amount, total, limit, skew), jnp.int32)
    couples = (amount - 1) // 2
    source_of, receiver = sizes[1:1 + 2 * couples:2], sizes[2:2 + 2 * couples:2]
    room = jnp.minimum(source_of - 1, limit - receiver)
    moved = jax.random.randint(jax.random.fold_in(key, 1), (couples,), 0, 1 << 20) % (room + 1)
    sizes = sizes.at[1:1 + 2 * couples:2].set(source_of - moved).at[2:2 + 2 * couples:2].set(receiver + moved)
    return sizes[jax.random.permutation(jax.random.fold_in(key, 2), amount)]


def normal_values(stream_key, extent, scale, most, shards=(), held_as=jnp.bfloat16):
    result = jax.random.normal(stream_key, extent, jnp.float32) * scale
    if len(shards) > 0:
        result = steps_of(stream_key, extent, shards, -0.22, 0.18) * result
    return jnp.clip(result, min=-most, max=most).astype(held_as)


def setup_inputs(seed: int = 0) -> dict:
    arg_keys = jax.random.split(jax.random.key(seed), 9)
    return {
        "visual_hidden": normal_values(arg_keys[0], (SEQUENCE_COUNT, MAXV, MODEL_WIDTH), 1.0, 6.0, ((0, 2), (1, 4), (2, 4))),
        "projector_weight": normal_values(arg_keys[1], (MODEL_WIDTH, MODEL_WIDTH), MODEL_WIDTH ** -0.5, 0.078125, ((0, 4),)),
        "text_embeddings": normal_values(arg_keys[2], (SEQUENCE_COUNT, SEQUENCE_LENGTH, MODEL_WIDTH), 1.0, 6.0, ((0, 8), (1, 4))),
        "tile_counts": uneven(arg_keys[3], SEQUENCE_COUNT, TILES, MAXT, 2).astype(jnp.int32),
        "image_start": place_ends(jax.random.randint(arg_keys[4], (SEQUENCE_COUNT,), 0, SEQUENCE_LENGTH - MAXV + 1), jax.random.fold_in(arg_keys[4], 1), 0, SEQUENCE_LENGTH - MAXV).astype(jnp.int32),
        "norm_gain": jnp.clip(1.0 + 0.1 * jax.random.normal(arg_keys[5], (MODEL_WIDTH,), jnp.float32), 0.5, 1.5),
        "query_weight": draw_query_weight(jax.random.fold_in(arg_keys[8], 71), 0),
        "keyvalue_weight": draw_keyvalue_weight(jax.random.fold_in(arg_keys[8], 71), 0),
    }


epsilon = 1e-06
masked_score = -1e+30

def attend_block(block_queries, first_row, keys, values):
    rows = block_queries.shape[0]
    scale = 1.0 / HEAD_SIZE ** 0.5
    scores = jnp.einsum('qkgd,rkd->kgqr', block_queries.astype(jnp.float32), keys.astype(jnp.float32)) * scale
    query_pos = first_row + jnp.arange(rows, dtype=jnp.int32)
    key_pos = jnp.arange(SEQUENCE_LENGTH, dtype=jnp.int32)
    causal_mask = key_pos[None, :] <= query_pos[:, None]
    scores = jnp.where(causal_mask, scores, masked_score)
    row_max = lax.optimization_barrier(jnp.max(scores, axis=-1, keepdims=True))
    expo = jnp.where(causal_mask, jnp.exp(scores - row_max), 0.0)
    denominator = lax.optimization_barrier(jnp.sum(expo, axis=-1))
    rounded = expo.astype(jnp.bfloat16)
    summed = jnp.einsum('kgqr,rkd->qkgd', rounded.astype(jnp.float32), values.astype(jnp.float32))
    summed = summed / jnp.transpose(denominator, (2, 0, 1))[..., None]
    return summed.astype(jnp.bfloat16).reshape(rows, QUERY_HEADS * HEAD_SIZE)

def reference(visual_hidden, projector_weight, text_embeddings, tile_counts, image_start, norm_gain, query_weight, keyvalue_weight):
    query_groups = QUERY_HEADS // KEY_VALUE_HEADS
    activated = jax.nn.gelu(visual_hidden.astype(jnp.float32), approximate=False).astype(jnp.bfloat16)
    visual = jnp.dot(activated, projector_weight, preferred_element_type=jnp.float32).astype(jnp.bfloat16)
    positions = jnp.arange(SEQUENCE_LENGTH, dtype=jnp.int32)
    slot_index = positions[None, :] - image_start[:, None].astype(jnp.int32)
    inside = (slot_index >= 0) & (slot_index < TILE * tile_counts[:, None].astype(jnp.int32))
    clipped = jnp.clip(slot_index, 0, MAXV - 1).astype(jnp.int32)
    placed = jnp.take_along_axis(visual, clipped[:, :, None], axis=1)
    mixed = jnp.where(inside[:, :, None], placed, text_embeddings)
    widened = mixed.astype(jnp.float32)
    mean_square = lax.optimization_barrier(jnp.mean(widened * widened, axis=-1, keepdims=True))
    normed = (widened * lax.rsqrt(mean_square + epsilon) * norm_gain).astype(jnp.bfloat16)
    flat = normed.reshape(SEQUENCE_COUNT * SEQUENCE_LENGTH, MODEL_WIDTH)
    query_rows = jnp.dot(flat, query_weight, preferred_element_type=jnp.float32).astype(jnp.bfloat16)
    key_value_rows = jnp.dot(flat, keyvalue_weight, preferred_element_type=jnp.float32).astype(jnp.bfloat16)
    query_rows = query_rows.reshape(SEQUENCE_COUNT, SEQUENCE_LENGTH, KEY_VALUE_HEADS, query_groups, HEAD_SIZE)
    key_value_rows = key_value_rows.reshape(SEQUENCE_COUNT, SEQUENCE_LENGTH, 2, KEY_VALUE_HEADS, HEAD_SIZE)
    block_current = min(512, SEQUENCE_LENGTH)

    def one_sequence(operands):
        sequence_query_rows, seq_keyvalues = operands
        keys = seq_keyvalues[:, 0]
        values = seq_keyvalues[:, 1]
        block_split = sequence_query_rows.reshape(SEQUENCE_LENGTH // block_current, block_current, KEY_VALUE_HEADS, query_groups, HEAD_SIZE)
        starts = jnp.arange(SEQUENCE_LENGTH // block_current, dtype=jnp.int32) * block_current
        return lax.map(lambda item: attend_block(item[0], item[1], keys, values), (block_split, starts)).reshape(SEQUENCE_LENGTH, QUERY_HEADS * HEAD_SIZE)
    return lax.map(one_sequence, (query_rows, key_value_rows))
```

```python
import functools
import math

import jax
import jax.numpy as jnp
from jax import lax
from jax.experimental import pallas as pl
from jax.experimental.layout import Layout, with_layout_constraint
from jax.experimental.pallas import tpu as pltpu
from jax.sharding import PartitionSpec as P

QUERY_HEADS = 20
KEY_VALUE_HEADS = 4
HEAD_SIZE = 128
TILE = 256


epsilon = 1e-06
masked_score = -1e30
QUERY_GROUPS = QUERY_HEADS // KEY_VALUE_HEADS


def distances(count):
    steps = []
    step = count // 2
    while step >= 1:
        steps.append(step)
        step = step // 2
    return steps


def swap(value, axis, step):
    count = lax.axis_size(axis)
    return lax.ppermute(value, axis, [(i, i ^ step) for i in range(count)])


def spread(piece, links):
    pieces = {0: piece}
    for bit, axis, step in links:
        for key, value in list(pieces.items()):
            pieces[key | bit] = swap(value, axis, step)
    return pieces


def attention_kernel(info_ref, q_ref, k_ref, v_ref, *refs, key_block, row_block):
    o_ref, max_ref, sum_ref, acc_ref = refs[-4:]
    rows = q_ref.shape[0]
    first_row = info_ref[0]
    full_blocks = first_row // key_block
    factor = math.log2(math.e) / math.sqrt(HEAD_SIZE)
    max_ref[...] = jnp.full(max_ref.shape, masked_score, jnp.float32)
    sum_ref[...] = jnp.zeros(sum_ref.shape, jnp.float32)
    acc_ref[...] = jnp.zeros(acc_ref.shape, jnp.float32)
    lanes = max_ref.shape[-1]

    def absorb(block, masked):
        start = pl.multiple_of(block * key_block, key_block)
        keys = k_ref[pl.ds(start, key_block), :]
        values = v_ref[pl.ds(start, key_block), :]
        for part in range(rows // row_block):
            span = slice(part * row_block, (part + 1) * row_block)
            if masked:
                query_pos = first_row + part * row_block + lax.broadcasted_iota(
                    jnp.int32, (row_block, key_block), 0
                )
                key_pos = start + lax.broadcasted_iota(jnp.int32, (row_block, key_block), 1)
                keep = key_pos <= query_pos
            for g in range(QUERY_GROUPS):
                queries = q_ref[span, g * HEAD_SIZE : (g + 1) * HEAD_SIZE]
                scores = lax.dot_general(
                    queries, keys, (((1,), (1,)), ((), ())), preferred_element_type=jnp.float32
                )
                if masked:
                    scores = jnp.where(keep, scores, masked_score)
                old_max = max_ref[g, span, :]
                new_max = jnp.maximum(old_max, jnp.max(scores, axis=1, keepdims=True))
                scaled_max = new_max * factor
                expo = jnp.exp2(
                    scores * factor - jnp.concatenate([scaled_max] * (key_block // lanes), axis=1)
                )
                rescale = jnp.exp2(old_max * factor - scaled_max)
                max_ref[g, span, :] = new_max
                sum_ref[g, span, :] = sum_ref[g, span, :] * rescale + jnp.sum(
                    expo, axis=1, keepdims=True
                )
                added = jnp.dot(
                    expo.astype(jnp.bfloat16), values, preferred_element_type=jnp.float32
                )
                acc_ref[g, span, :] = acc_ref[g, span, :] * rescale + added

    def body(block, carry):
        absorb(block, False)
        return carry

    lax.fori_loop(0, full_blocks, body, 0)
    absorb(full_blocks, True)
    for g in range(QUERY_GROUPS):
        o_ref[:, g * HEAD_SIZE : (g + 1) * HEAD_SIZE] = (acc_ref[g] / sum_ref[g]).astype(o_ref.dtype)


def attend(first_row, queries, keyvalues, index, total_sequences, before):
    rows = queries.shape[0]
    total = keyvalues.shape[0]
    half_heads = KEY_VALUE_HEADS // 2
    wide = QUERY_GROUPS * HEAD_SIZE
    key_block = min(1024, total)
    row_block = min(512, rows)
    assert key_block % rows == 0 and rows % row_block == 0
    grid_spec = pltpu.PrefetchScalarGridSpec(
        num_scalar_prefetch=1,
        grid=(KEY_VALUE_HEADS,),
        in_specs=[
            pl.BlockSpec((rows, wide), lambda h, info: (0, h)),
            pl.BlockSpec(
                (total, HEAD_SIZE), lambda h, info: (0, h // half_heads * 2 * half_heads + h % half_heads)
            ),
            pl.BlockSpec(
                (total, HEAD_SIZE),
                lambda h, info: (0, h // half_heads * 2 * half_heads + half_heads + h % half_heads),
            ),
        ]
        + ([] if before is None else [pl.BlockSpec(memory_space=pl.ANY)]),
        out_specs=pl.BlockSpec((None, rows, wide), lambda h, info: (index, 0, h)),
        scratch_shapes=[
            pltpu.VMEM((QUERY_GROUPS, rows, HEAD_SIZE), jnp.float32),
            pltpu.VMEM((QUERY_GROUPS, rows, HEAD_SIZE), jnp.float32),
            pltpu.VMEM((QUERY_GROUPS, rows, HEAD_SIZE), jnp.float32),
        ],
    )
    pairs = QUERY_HEADS * rows * total
    return pl.pallas_call(
        functools.partial(attention_kernel, key_block=key_block, row_block=row_block),
        out_shape=jax.ShapeDtypeStruct((total_sequences, rows, QUERY_HEADS * HEAD_SIZE), jnp.bfloat16),
        input_output_aliases={} if before is None else {4: 0},
        grid_spec=grid_spec,
        name="attend",
        compiler_params=pltpu.CompilerParams(
            dimension_semantics=("arbitrary",), vmem_limit_bytes=40 * 1024 * 1024
        ),
        cost_estimate=pl.CostEstimate(
            flops=4 * pairs * HEAD_SIZE, transcendentals=pairs, bytes_accessed=2 * queries.size * 4
        ),
    )(first_row.reshape(1), queries, keyvalues, keyvalues, *([] if before is None else [before]))


def shards(
    visual_hidden,
    projector_weight,
    text_embeddings,
    tile_counts,
    image_start,
    norm_gain,
    query_weight,
    keyvalue_weight,
):
    tensor_count = lax.axis_size("tensoror")
    seq_count = lax.axis_size("seq")
    group_count = lax.axis_size("group")
    sequence_local, extent_rows, width = text_embeddings.shape
    slot_rows = visual_hidden.shape[1]
    features = visual_hidden.shape[2]
    slot_total = slot_rows * seq_count
    position_total = extent_rows * seq_count
    tensor_rank = lax.axis_index("tensoror")
    seq_rank = lax.axis_index("seq")
    group_rank = lax.axis_index("group")
    core = seq_rank % 2
    plane_count = group_count * (seq_count // 2)
    plane_rank = group_rank * (seq_count // 2) + seq_rank // 2
    query_cols = query_weight.shape[1]
    pair_cols = keyvalue_weight.shape[1]
    query_half = query_cols // 2
    pair_half = pair_cols // 2

    piece_rows = features // plane_count
    links = []
    bit = 1
    for step in reversed(distances(seq_count)):
        if step > 1:
            links.append((bit, "seq", step))
            bit *= 2
    for step in reversed(distances(group_count)):
        links.append((bit, "group", step))
        bit *= 2

    def fetch(local, share):
        cols = local.shape[1]
        piece = lax.dynamic_slice_in_dim(local, plane_rank * piece_rows, piece_rows, 0)
        return local, lax.all_gather(piece, "tensoror", axis=0), share

    def pass_on(local, gathered, share):
        cols = local.shape[1]
        foreign = lax.dynamic_slice_in_dim(
            jnp.concatenate([gathered, gathered], axis=0), tensor_rank + 1, tensor_count - 1, 0
        )
        cut = max(128, int(cols * share) // 128 * 128)
        first = spread(foreign[:, :, :cut], links)
        second = spread(foreign[:, :, cut:], links[::-1])
        return local, cut, first, second

    def assemble(local, cut, first, second):
        cols = local.shape[1]
        whole = jnp.zeros((tensor_count, plane_count, piece_rows, cols), local.dtype)
        whole = lax.dynamic_update_slice(
            whole, local.reshape(1, plane_count, piece_rows, cols), (0, 0, 0, 0)
        )
        for key in range(plane_count):
            order = plane_rank ^ key
            whole = lax.dynamic_update_slice(whole, first[key][:, None], (1, order, 0, 0))
            whole = lax.dynamic_update_slice(whole, second[key][:, None], (1, order, 0, cut))
        own = whole.reshape(tensor_count * features, cols)
        return own, swap(own, "seq", 1)

    quarter = pair_half // 2
    pair_columns = [
        lax.dynamic_slice_in_dim(keyvalue_weight, core * quarter, quarter, 1),
        lax.dynamic_slice_in_dim(keyvalue_weight, pair_half + core * quarter, quarter, 1),
    ]
    query_columns = lax.dynamic_slice_in_dim(query_weight, core * query_half, query_half, 1)
    early = 2 * HEAD_SIZE
    fetched = [
        fetch(jnp.concatenate(pair_columns + [query_columns[:, :early]], axis=1), 0.5),
        fetch(query_columns[:, early:], 0.25),
    ]

    def roll(rows):
        return lax.dynamic_slice_in_dim(
            jnp.concatenate([rows, rows], axis=1), tensor_rank * features, width, 1
        )

    def multiply(rows, pair):
        own, other = (
            with_layout_constraint(
                jnp.dot(rows, weight, preferred_element_type=jnp.float32).astype(jnp.bfloat16),
                Layout(major_to_minor=(0, 1)),
            )
            for weight in pair
        )
        return jnp.where(core == 0, own, other), jnp.where(core == 0, other, own)

    def arrange(early_parts, late_parts):
        pairs = jnp.concatenate([part[:, :pair_half] for part in early_parts], axis=1)
        queries = jnp.concatenate(
            [early_parts[0][:, pair_half:], late_parts[0], early_parts[1][:, pair_half:], late_parts[1]],
            axis=1,
        )
        return queries, pairs

    def normalise(rows):
        widened = rows.astype(jnp.float32)
        mean_square = jnp.mean(widened * widened, axis=-1, keepdims=True)
        return (widened * lax.rsqrt(mean_square + epsilon) * norm_gain).astype(jnp.bfloat16)

    seq_links = []
    bit = 1
    for step in reversed(distances(seq_count)):
        seq_links.append((bit, "seq", step))
        bit *= 2

    def over_seq(rows, tie=None):
        far = seq_links[-1]
        pieces = {0: rows, far[0]: swap(rows, far[1], far[2])}
        if tie is not None:
            pieces[far[0]], tie = lax.optimization_barrier((pieces[far[0]], tie))
        for bit, axis, step in seq_links[-2::-1]:
            for key, value in list(pieces.items()):
                pieces[key | bit] = swap(value, axis, step)
        whole = jnp.zeros((seq_count,) + rows.shape, rows.dtype)
        for key in range(seq_count):
            whole = lax.dynamic_update_slice(
                whole, pieces[key][None], (seq_rank ^ key,) + (0,) * rows.ndim
            )
        return whole, tie

    activated = jax.nn.gelu(visual_hidden.astype(jnp.float32), approximate=False).astype(
        jnp.bfloat16
    )
    activated = lax.optimization_barrier(activated)
    activated = activated.reshape(tensor_count, sequence_local, slot_rows, features)
    partials = []
    for j in range(sequence_local):
        chunk = activated[:, j]
        if partials:
            chunk, partial = lax.optimization_barrier((chunk, partial))
        partial = jnp.dot(
            chunk.reshape(tensor_count * slot_rows, features),
            projector_weight,
            preferred_element_type=jnp.float32,
        ).astype(jnp.bfloat16)
        partials.append(partial)

    early_local, early_gathered, early_share = fetched[0]
    early_gathered, partials = lax.optimization_barrier((early_gathered, partials))
    visual = [
        lax.psum_scatter(partial, "tensoror", scatter_dimension=0, tiled=True)
        for partial in partials
    ]
    early_local, early_cut, *early_pieces = pass_on(early_local, early_gathered, early_share)
    late_local, late_cut, *late_pieces = pass_on(*fetched[1])

    text = roll(normalise(text_embeddings).reshape(sequence_local * extent_rows, width))
    early_pieces, text = lax.optimization_barrier((early_pieces, text))
    early_weights = assemble(early_local, early_cut, *early_pieces)
    early_text = multiply(text, early_weights)
    late_pieces, early_text = lax.optimization_barrier((late_pieces, early_text))
    late_weights = assemble(late_local, late_cut, *late_pieces)
    late_text = multiply(text, late_weights)
    text_queries, text_pairs = arrange(early_text, late_text)
    text_queries = text_queries.reshape(sequence_local, extent_rows, query_cols)
    text_pairs = text_pairs.reshape(sequence_local, extent_rows, pair_cols)
    every_pair = []
    for j in range(sequence_local):
        gathered, text_queries = over_seq(text_pairs[j], text_queries)
        every_pair.append(gathered)

    image = []
    visual[0], text_queries = lax.optimization_barrier((visual[0], text_queries))
    for j in range(sequence_local):
        rows = roll(normalise(visual[j]))
        both = jnp.concatenate(
            arrange(multiply(rows, early_weights), multiply(rows, late_weights)), axis=1
        )
        if j == 0 and sequence_local > 1:
            both, visual[1] = over_seq(both, visual[1])
        image.append(both)

    first_seq = (group_rank * tensor_count + tensor_rank) * sequence_local
    first_row = seq_rank * extent_rows
    positions = first_row + jnp.arange(extent_rows, dtype=jnp.int32)
    slots = jnp.arange(slot_total, dtype=jnp.int32)
    result = None
    for j in range(sequence_local):
        count = lax.dynamic_index_in_dim(tile_counts, first_seq + j, keepdims=False)
        start = lax.dynamic_index_in_dim(image_start, first_seq + j, keepdims=False)
        both = image[j]
        if j > 0:
            both, result = over_seq(both, result)
        elif sequence_local == 1:
            both, result = over_seq(both)
        both = both.reshape(slot_total, query_cols + pair_cols)
        pairs = every_pair[j].reshape(position_total, pair_cols)
        window = lax.dynamic_slice_in_dim(pairs, start, slot_total, 0)
        window = jnp.where((slots < TILE * count)[:, None], both[:, query_cols:], window)
        pairs = lax.dynamic_update_slice_in_dim(pairs, window, start, 0)
        padded = jnp.pad(both[:, :query_cols], ((extent_rows, extent_rows), (0, 0)))
        offset = jnp.clip(first_row - start + extent_rows, 0, slot_total + extent_rows)
        shifted = lax.dynamic_slice_in_dim(padded, offset, extent_rows, 0)
        slot_index = positions - start
        inside = (slot_index >= 0) & (slot_index < TILE * count)
        queries = jnp.where(inside[:, None], shifted, text_queries[j])
        result = attend(first_row, queries, pairs, j, sequence_local, result)
    return result


def solution(mesh):
    in_specs = (
        P("group", "seq", "tensoror"),
        P("tensoror", None),
        P(("group", "tensoror"), "seq", None),
        P(),
        P(),
        P(),
        P("tensoror", None),
        P("tensoror", None),
    )
    out_specs = P(("group", "tensoror"), "seq", None)
    return jax.shard_map(shards, mesh=mesh, in_specs=in_specs, out_specs=out_specs, check_vma=False)
```
